8 devices in a mesh: dp: 1 (over z), sp: 2 (over y), cp: 4 (over x, core).
Axes of the slice: x: 2, y: 2, z: 1, core: 2. Of those that a mesh axis runs over, the one named last changes fastest.
Arguments:
- x_chunk: bfloat16 [4096, 3072], P(('dp', 'sp', 'cp'))
- k_cache: bfloat16 [4096, 8, 128], P(('dp', 'sp', 'cp'))
- v_cache: bfloat16 [4096, 8, 128], P(('dp', 'sp', 'cp'))
- w_q: bfloat16 [3072, 3072], replicated
- w_k: bfloat16 [3072, 1024], replicated
- w_v: bfloat16 [3072, 1024], replicated
- w_o: bfloat16 [3072, 3072], replicated
Outputs:
- output 1: bfloat16 [4096, 3072], P(('dp', 'sp', 'cp'))
- output 2: bfloat16 [4096, 8, 128], P(('dp', 'sp', 'cp'))
- output 3: bfloat16 [4096, 8, 128], P(('dp', 'sp', 'cp'))
All inputs are finite; a program needn't handle non-finite values.
Results may differ from the reference program's by a relative error of at most 0.00496302.
Values are sent between devices in bfloat16 or wider.
A program may use at most 1 GiB of HBM per device.

```python
import math
import jax
import jax.numpy as jnp
from jax import lax

D_MODEL = 3072
HEADS = 24
KV_HEADS = 8
HEAD = 128
TOK = 4096
CACHE = 4096
SHARDS = 8
QBLOCK = 16
ROPE_BASE = 500000


def rope_tables(positions):
    inv_freq = 1.0 / (ROPE_BASE ** (jnp.arange(0, HEAD, 2, dtype=jnp.float32) / HEAD))
    angles = positions.astype(jnp.float32)[:, None] * inv_freq[None, :]
    return jnp.cos(angles), jnp.sin(angles)


def apply_rope(values, cos_t, sin_t):
    half_dim = HEAD // 2
    lo_half = values[..., :half_dim].astype(jnp.float32)
    hi_half = values[..., half_dim:].astype(jnp.float32)
    return jnp.concatenate([lo_half * cos_t - hi_half * sin_t, hi_half * cos_t + lo_half * sin_t], axis=-1).astype(jnp.bfloat16)


def setup_inputs(seed: int = 0, part: int = 0) -> dict:
    group_size = HEADS // KV_HEADS
    shard_len = CACHE // SHARDS
    score_gap = max(1.0, math.log(CACHE / TOK) + 1.0)
    shared_keys = jax.random.split(jax.random.key(seed), 7)
    part_keys = jax.random.split(jax.random.fold_in(jax.random.key(seed + 1), part), 5)
    x_mean = 0.6 * jax.random.normal(shared_keys[0], (D_MODEL,), jnp.float32)
    low_dims = (jnp.arange(HEAD) % (HEAD // 2)) >= (HEAD // 2 - 8)
    bias_dir = jax.random.normal(shared_keys[1], (KV_HEADS, HEAD), jnp.float32) * low_dims
    bias_kv = bias_dir / jnp.linalg.norm(bias_dir, axis=-1, keepdims=True) * math.sqrt(score_gap * math.sqrt(HEAD))
    bias_q = jnp.repeat(bias_kv, group_size, axis=0).reshape(HEADS * HEAD)
    mean_lift = x_mean[:, None] / jnp.sum(x_mean * x_mean)
    w_q = jax.random.normal(shared_keys[2], (D_MODEL, HEADS * HEAD), jnp.float32) * D_MODEL ** -0.5 + mean_lift * bias_q[None, :]
    w_k = jax.random.normal(shared_keys[3], (D_MODEL, KV_HEADS * HEAD), jnp.float32) * D_MODEL ** -0.5 + mean_lift * bias_kv.reshape(KV_HEADS * HEAD)[None, :]
    w_v = jax.random.normal(shared_keys[4], (D_MODEL, KV_HEADS * HEAD), jnp.float32) * D_MODEL ** -0.5
    w_o = jax.random.normal(shared_keys[5], (HEADS * HEAD, D_MODEL), jnp.float32) * (HEADS * HEAD) ** -0.5
    x_chunk = 0.8 * jax.random.normal(part_keys[0], (TOK, D_MODEL), jnp.float32) + x_mean[None, :]
    key_scale = jnp.exp(jax.random.uniform(part_keys[1], (SHARDS, 1, 1, 1), jnp.float32, -0.7, 0.7)) / math.sqrt(1.0 + score_gap / math.sqrt(HEAD))
    k_cache = (jax.random.normal(part_keys[2], (SHARDS, shard_len, KV_HEADS, HEAD), jnp.float32) * key_scale).reshape(CACHE, KV_HEADS, HEAD)
    val_mean = jax.random.normal(part_keys[3], (SHARDS, 1, KV_HEADS, HEAD), jnp.float32)
    v_cache = (0.5 * jax.random.normal(part_keys[4], (SHARDS, shard_len, KV_HEADS, HEAD), jnp.float32) + val_mean).reshape(CACHE, KV_HEADS, HEAD)
    return {'x_chunk': x_chunk.astype(jnp.bfloat16), 'k_cache': k_cache.astype(jnp.bfloat16), 'v_cache': v_cache.astype(jnp.bfloat16), 'w_q': w_q.astype(jnp.bfloat16), 'w_k': w_k.astype(jnp.bfloat16), 'w_v': w_v.astype(jnp.bfloat16), 'w_o': w_o.astype(jnp.bfloat16)}


def reference(x_chunk, k_cache, v_cache, w_q, w_k, w_v, w_o):
    group_size = HEADS // KV_HEADS
    attn_scale = HEAD ** -0.5
    cos_t, sin_t = rope_tables(CACHE + jnp.arange(TOK))
    q_rows = jnp.dot(x_chunk, w_q, preferred_element_type=jnp.float32).astype(jnp.bfloat16)
    q_heads = apply_rope(q_rows.reshape(TOK, KV_HEADS, group_size, HEAD), cos_t[:, None, None, :], sin_t[:, None, None, :])
    k_rows = jnp.dot(x_chunk, w_k, preferred_element_type=jnp.float32).astype(jnp.bfloat16)
    k_new = apply_rope(k_rows.reshape(TOK, KV_HEADS, HEAD), cos_t[:, None, :], sin_t[:, None, :])
    v_new = jnp.dot(x_chunk, w_v, preferred_element_type=jnp.float32).astype(jnp.bfloat16).reshape(TOK, KV_HEADS, HEAD)
    keys_all = jnp.concatenate([k_cache, k_new], axis=0)
    vals_all = jnp.concatenate([v_cache, v_new], axis=0)
    key_pos = jnp.arange(CACHE + TOK)
    block_starts = jnp.arange(TOK // QBLOCK) * QBLOCK

    def per_head(head_args):
        q_head, k_head, v_head = head_args
        k_trans = k_head.T

        def per_block(block_args):
            q_block, row_start = block_args
            scores = jnp.dot(q_block.reshape(QBLOCK * group_size, HEAD), k_trans, preferred_element_type=jnp.float32)
            scores = scores.reshape(QBLOCK, group_size, CACHE + TOK) * attn_scale
            allowed = key_pos[None, None, :] <= (CACHE + row_start + jnp.arange(QBLOCK))[:, None, None]
            scores = jnp.where(allowed, scores, -jnp.inf)
            row_max = jnp.max(scores, axis=-1, keepdims=True)
            exp_scores = jnp.exp(scores - row_max)
            row_sum = jnp.sum(exp_scores, axis=-1, keepdims=True)
            out_block = jnp.dot(exp_scores.astype(jnp.bfloat16).reshape(QBLOCK * group_size, CACHE + TOK), v_head, preferred_element_type=jnp.float32)
            return out_block.reshape(QBLOCK, group_size, HEAD) / row_sum

        blocks = lax.map(per_block, (q_head.reshape(TOK // QBLOCK, QBLOCK, group_size, HEAD), block_starts))
        return blocks.reshape(TOK, group_size, HEAD)

    attn_out = lax.map(per_head, (jnp.transpose(q_heads, (1, 0, 2, 3)), jnp.transpose(keys_all, (1, 0, 2)), jnp.transpose(vals_all, (1, 0, 2))))
    attn_rows = jnp.transpose(attn_out, (1, 0, 2, 3)).reshape(TOK, HEADS * HEAD).astype(jnp.bfloat16)
    y_out = jnp.dot(attn_rows, w_o, preferred_element_type=jnp.float32).astype(jnp.bfloat16)
    return (y_out, k_new, v_new)
```

```python
import functools

import jax
import jax.numpy as jnp
from jax import lax
from jax.experimental import pallas as pl
from jax.experimental.pallas import tpu as pltpu
from jax.sharding import PartitionSpec as P

ROPE_BASE = 500000
MESH_ID = pl.DeviceIdType.MESH
NDEV = 8
NEG = -1e30
LOG2E = 1.4426950408889634
KC, VC, QN, KN, VN = range(5)


def rope_tables(positions, head_dim):
    inv_freq = 1.0 / (ROPE_BASE ** (jnp.arange(0, head_dim, 2, dtype=jnp.float32) / head_dim))
    angles = positions.astype(jnp.float32)[:, None] * inv_freq[None, :]
    return jnp.cos(angles), jnp.sin(angles)


def apply_rope(values, cos_t, sin_t):
    half_dim = values.shape[-1] // 2
    lo_half = values[..., :half_dim].astype(jnp.float32)
    hi_half = values[..., half_dim:].astype(jnp.float32)
    return jnp.concatenate([lo_half * cos_t - hi_half * sin_t, hi_half * cos_t + lo_half * sin_t], axis=-1).astype(jnp.bfloat16)


def attn_kernel(group, tok, scale, q_hbm, kn_hbm, vn_hbm, kc_hbm, vc_hbm, o_hbm,
                q_s, kc_s, vc_s, kn_s, vn_s, acc, m_s, l_s, s_s, osend, send_sem, recv_sem, osend_sem, orecv_sem):
    y = lax.axis_index('sp')
    xc = lax.axis_index('cp')
    x, c = xc // 2, xc % 2
    me = y * 4 + xc
    c2 = scale * LOG2E
    hd = 128
    gw = group * hd

    def peer(k):
        py, px, pc = (y + k // 4) % 2, (x + (k // 2) % 2) % 2, (c + k % 2) % 2
        return py * 4 + px * 2 + pc, (0, py, px * 2 + pc)

    barrier = pltpu.get_barrier_semaphore()
    for k in range(1, NDEV):
        pl.semaphore_signal(barrier, inc=1, device_id=peer(k)[1], device_id_type=MESH_ID)
    srcs = (kc_hbm, vc_hbm, q_hbm, kn_hbm, vn_hbm)
    dsts = (kc_s, vc_s, q_s, kn_s, vn_s)

    def local(kind):
        slot = me if kind in (KN, VN) else 0
        return pltpu.make_async_copy(srcs[kind].at[me], dsts[kind].at[slot], recv_sem.at[kind, 0])

    def remote(kind, k):
        p, did = peer(k)
        slot = me if kind in (KN, VN) else k
        return pltpu.make_async_remote_copy(src_ref=srcs[kind].at[p], dst_ref=dsts[kind].at[slot], send_sem=send_sem.at[kind, k],
                                            recv_sem=recv_sem.at[kind, k], device_id=did, device_id_type=MESH_ID)

    def arrived(kind, k):
        slot = peer(k)[0] if kind in (KN, VN) else k
        pltpu.make_async_copy(srcs[kind].at[0], dsts[kind].at[slot], recv_sem.at[kind, k]).wait()

    for kind in range(5):
        local(kind).start()
    acc[...] = jnp.zeros_like(acc)
    l_s[...] = jnp.zeros_like(l_s)
    m_s[...] = jnp.full(m_s.shape, NEG, jnp.float32)
    pl.semaphore_wait(barrier, NDEV - 1)
    order = (1, 2, 4, 6, 3, 5, 7)
    for kinds in ((KC, VC), (QN,), (KN, VN)):
        for k in order:
            for kind in kinds:
                remote(kind, k).start()

    def qk(keys, k, r):
        return lax.dot_general(keys, q_s[k, r * tok:(r + 1) * tok, :], (((1,), (1,)), ((), ())), preferred_element_type=jnp.float32)

    def soft_pv(k, r, s, mx, vt):
        cols = slice(r * tok, (r + 1) * tok)
        m_old = m_s[k, :, cols]
        m_new = jnp.maximum(m_old, mx * c2)
        m_s[k, :, cols] = m_new
        alpha = jnp.exp2(m_old - m_new)
        p = jnp.exp2(s * c2 - m_new)
        l_s[k, :, cols] = l_s[k, :, cols] * alpha + jnp.sum(p, axis=0, keepdims=True)
        pv = lax.dot_general(vt, p.astype(jnp.bfloat16), (((1,), (0,)), ((), ())), preferred_element_type=jnp.float32)
        acc[k, :, cols] = acc[k, :, cols] * alpha + pv

    def kchunk(j):
        return kc_s[pl.ds(2 * j, 2)].reshape(2 * tok, hd)

    def vpv(k, r, s, mx, j):
        vt = jnp.concatenate([vc_s[2 * j], vc_s[2 * j + 1]], axis=1)
        soft_pv(k, r, s, mx, vt)

    for kind, k in ((KC, 0), (KC, 1), (QN, 0), (VC, 0), (VC, 1)):
        arrived(kind, k)
    s0 = qk(kchunk(0), 0, 0)
    s_s[0] = s0
    n1 = NDEV * 4

    def phase1(t, mx):
        k, j = t // 4, t % 4
        tn = jnp.minimum(t + 1, n1 - 1)
        kn_, jn_ = tn // 4, tn % 4

        @pl.when(jnp.logical_and(k == 0, j < 3))
        def _():
            for kind in (KC, VC):
                arrived(kind, 2 * jn_)
                arrived(kind, 2 * jn_ + 1)

        @pl.when(jnp.logical_and(j == 3, k < NDEV - 1))
        def _():
            arrived(QN, kn_)

        for r in range(group):
            nr = (r + 1) % group
            s_next = qk(kchunk(j), k, nr) if nr else qk(kchunk(jn_), kn_, 0)
            cur = s_s[r]
            s_s[nr] = s_next
            vpv(k, r, cur, mx, j)
            mx = jnp.max(s_next, axis=0, keepdims=True)
        return mx

    lax.fori_loop(0, n1, phase1, jnp.max(s0, axis=0, keepdims=True))

    for k in range(NDEV):
        arrived(KN, k)
        arrived(VN, k)
    ahead = lax.broadcasted_iota(jnp.int32, (tok, tok), 0) <= lax.broadcasted_iota(jnp.int32, (tok, tok), 1)
    half = pl.ds(0, tok)

    def owner_cols(dev):
        return pl.ds(pl.multiple_of(dev * gw, gw), gw)

    def send_out(k):
        return pltpu.make_async_remote_copy(src_ref=osend.at[k], dst_ref=o_hbm.at[:, owner_cols(me)], send_sem=osend_sem.at[k],
                                            recv_sem=orecv_sem.at[k], device_id=peer(k)[1], device_id_type=MESH_ID)

    def phase2(kk, carry):
        k = NDEV - 1 - kk
        p = peer(k)[0]
        s = jnp.where(ahead, qk(kn_s[p], k, 0), NEG)
        s_s[0, half] = s
        mx = jnp.max(s, axis=0, keepdims=True)
        for r in range(group):
            nr = (r + 1) % group
            s_next = jnp.where(ahead, qk(kn_s[p], k, nr), NEG) if nr else qk(kn_s[0], k, 0)
            cur = s_s[r, half]
            s_s[nr, half] = s_next
            soft_pv(k, r, cur, mx, vn_s[p])
            mx = jnp.max(s_next, axis=0, keepdims=True)

        @pl.when(kk > 0)
        def _():
            send_out(k + 1).start()

        def earlier(j, mx):
            jn = jnp.minimum(j + 1, p - 1)
            for r in range(group):
                nr = (r + 1) % group
                s_next = qk(kn_s[j], k, nr) if nr else qk(kn_s[jn], k, 0)
                cur = s_s[r, half]
                s_s[nr, half] = s_next
                soft_pv(k, r, cur, mx, vn_s[j])
                mx = jnp.max(s_next, axis=0, keepdims=True)
            return mx

        lax.fori_loop(0, p, earlier, mx)
        for r in range(group):
            cols = slice(r * tok, (r + 1) * tok)
            o_t = acc[k, :, cols] * (1.0 / l_s[k, :, cols])
            osend[k, :, r * hd:(r + 1) * hd] = o_t.T.astype(jnp.bfloat16)
        return carry

    lax.fori_loop(0, NDEV, phase2, 0)
    own = pltpu.make_async_copy(osend.at[0], o_hbm.at[:, owner_cols(me)], orecv_sem.at[0])
    own.start()
    for k in range(1, NDEV):
        for kind in range(5):
            remote(kind, k).wait_send()
        send_out(k).wait_send()
        pltpu.make_async_copy(osend.at[k], o_hbm.at[:, owner_cols(peer(k)[0])], orecv_sem.at[k]).wait()
    own.wait()


def attention(q_t, kn_t, vn_t, kc_t, vc_t):
    kv_heads, rows, hd = q_t.shape
    tok = kn_t.shape[1]
    group = rows // tok
    bf, f32 = jnp.bfloat16, jnp.float32
    hbm = pl.BlockSpec(memory_space=pl.ANY)
    return pl.pallas_call(
        functools.partial(attn_kernel, group, tok, hd ** -0.5),
        out_shape=jax.ShapeDtypeStruct((tok, kv_heads * group * hd), bf),
        in_specs=[hbm] * 5,
        out_specs=hbm,
        scratch_shapes=[
            pltpu.VMEM((NDEV, rows, hd), bf),
            pltpu.VMEM((NDEV, tok, hd), bf),
            pltpu.VMEM((NDEV, hd, tok), bf),
            pltpu.VMEM((NDEV, tok, hd), bf),
            pltpu.VMEM((NDEV, hd, tok), bf),
            pltpu.VMEM((NDEV, hd, rows), f32),
            pltpu.VMEM((NDEV, 1, rows), f32),
            pltpu.VMEM((NDEV, 1, rows), f32),
            pltpu.VMEM((group, 2 * tok, tok), f32),
            pltpu.VMEM((NDEV, tok, group * hd), bf),
            pltpu.SemaphoreType.DMA((5, NDEV)),
            pltpu.SemaphoreType.DMA((5, NDEV)),
            pltpu.SemaphoreType.DMA((NDEV,)),
            pltpu.SemaphoreType.DMA((NDEV,)),
        ],
        compiler_params=pltpu.CompilerParams(collective_id=0, has_side_effects=True, vmem_limit_bytes=56 * 2**20),
        name='head_attention',
    )(q_t, kn_t, vn_t, kc_t, vc_t)


def solution(mesh):
    seq_size = mesh.shape['sp'] * mesh.shape['cp']
    cp_size = mesh.shape['cp']
    row_spec = P(('dp', 'sp', 'cp'))

    def local_fn(x_loc, kc_loc, vc_loc, w_q, w_k, w_v, w_o):
        tok, d_model = x_loc.shape
        cache_loc, kv_heads, hd = kc_loc.shape
        group = w_q.shape[1] // (kv_heads * hd)
        seq_idx = lax.axis_index('sp') * cp_size + lax.axis_index('cp')
        kc_t = jnp.transpose(kc_loc, (1, 0, 2))
        vc_t = jnp.transpose(vc_loc, (1, 2, 0))
        cos_t, sin_t = rope_tables(cache_loc * seq_size + seq_idx * tok + jnp.arange(tok), hd)
        k_rows = jnp.dot(x_loc, w_k, preferred_element_type=jnp.float32).astype(jnp.bfloat16)
        k_new = apply_rope(k_rows.reshape(tok, kv_heads, hd), cos_t[:, None, :], sin_t[:, None, :])
        v_new = jnp.dot(x_loc, w_v, preferred_element_type=jnp.float32).astype(jnp.bfloat16).reshape(tok, kv_heads, hd)
        q_rows = jnp.dot(x_loc, w_q, preferred_element_type=jnp.float32).astype(jnp.bfloat16)
        q_t = jnp.transpose(q_rows.reshape(tok, kv_heads, group, hd), (1, 2, 0, 3))
        q_t = apply_rope(q_t, cos_t, sin_t).reshape(kv_heads, group * tok, hd)
        o_rows = attention(q_t, jnp.transpose(k_new, (1, 0, 2)), jnp.transpose(v_new, (1, 2, 0)), kc_t, vc_t)
        y_loc = jnp.dot(o_rows, w_o, preferred_element_type=jnp.float32).astype(jnp.bfloat16)
        return y_loc, k_new, v_new

    return jax.shard_map(local_fn, mesh=mesh, in_specs=(row_spec, row_spec, row_spec, P(), P(), P(), P()), out_specs=(row_spec, row_spec, row_spec), check_vma=False)
```

```python
import functools

import jax
import jax.numpy as jnp
from jax import lax
from jax.experimental import pallas as pl
from jax.experimental.pallas import tpu as pltpu
from jax.sharding import PartitionSpec as P

ROPE_BASE = 500000
MESH_ID = pl.DeviceIdType.MESH
NDEV = 8
NEG = -1e30
LOG2E = 1.4426950408889634
KC, VC, QN, KN, VN = range(5)
NBUF = 3


def rope_tables(positions, head_dim):
    half = jnp.arange(head_dim) % (head_dim // 2)
    inv_freq = 1.0 / (ROPE_BASE ** ((2 * half).astype(jnp.float32) / head_dim))
    angles = positions.astype(jnp.float32)[:, None] * inv_freq[None, :]
    sign = jnp.where(jnp.arange(head_dim) < head_dim // 2, -1.0, 1.0)
    return jnp.cos(angles), jnp.sin(angles) * sign


def layer_kernel(group, tok, scale, x_hbm, wq_hbm, wk_hbm, wv_hbm, cos_hbm, sin_hbm, kc_hbm, vc_hbm, o_hbm, ko_hbm, vo_hbm,
                 x_s, cos_s, sin_s, wbuf, q_send, k_rows, v_rows, q_s, kc_s, vc_raw, vc_t, kn_s, vn_raw, vn_t, acc, m_s, l_s, s_s, osend,
                 in_sem, w_sem, send_sem, recv_sem, osend_sem, orecv_sem):
    y = lax.axis_index('sp')
    xc = lax.axis_index('cp')
    x, c = xc // 2, xc % 2
    me = y * 4 + xc
    c2 = scale * LOG2E
    hd = cos_s.shape[1]
    gw = group * hd
    wide = wbuf.shape[2]

    def peer(k):
        py, px, pc = (y + k // 4) % 2, (x + (k // 2) % 2) % 2, (c + k % 2) % 2
        return py * 4 + px * 2 + pc, (0, py, px * 2 + pc)

    def head_cols(dev):
        return pl.ds(pl.multiple_of(dev * hd, hd), hd)

    def group_cols(dev):
        return pl.ds(pl.multiple_of(dev * gw, gw), gw)

    barrier = pltpu.get_barrier_semaphore()
    for k in range(1, NDEV):
        pl.semaphore_signal(barrier, inc=1, device_id=peer(k)[1], device_id_type=MESH_ID)

    def q_chip(i):
        kc = (i + 1) % 4
        return ((y + kc // 2) % 2) * 2 + (x + kc % 2) % 2

    def w_copy(w_hbm, col, width, t):
        return pltpu.make_async_copy(w_hbm.at[:, pl.ds(pl.multiple_of(col, 256), width)], wbuf.at[t % NBUF, :, pl.ds(0, width)], w_sem.at[t % NBUF])

    def wq_tile(i):
        return w_copy(wq_hbm, q_chip(i) * wide, wide, i)

    def wk_tile(i):
        return w_copy(wk_hbm, i * 512, 512, 4 + i)

    def wv_tile(i):
        return w_copy(wv_hbm, i * 512, 512, 6 + i)

    loads = [pltpu.make_async_copy(x_hbm, x_s, in_sem.at[0]), pltpu.make_async_copy(cos_hbm, cos_s, in_sem.at[1]), pltpu.make_async_copy(sin_hbm, sin_s, in_sem.at[2])]
    loads[0].start()
    wq_tile(0).start()
    loads[1].start()
    loads[2].start()
    wq_tile(1).start()

    def src(kind, dev):
        if kind in (KN, VN):
            return (k_rows if kind == KN else v_rows).at[:, head_cols(dev)]
        return {KC: kc_hbm, VC: vc_hbm, QN: q_send}[kind].at[dev]

    dsts = (kc_s, vc_raw, q_s, kn_s, vn_raw)

    def local(kind):
        slot = me if kind in (KN, VN) else 0
        return pltpu.make_async_copy(src(kind, me), dsts[kind].at[slot], recv_sem.at[kind, 0])

    def remote(kind, k):
        p, did = peer(k)
        slot = me if kind in (KN, VN) else k
        return pltpu.make_async_remote_copy(src_ref=src(kind, p), dst_ref=dsts[kind].at[slot], send_sem=send_sem.at[kind, k],
                                            recv_sem=recv_sem.at[kind, k], device_id=did, device_id_type=MESH_ID)

    def arrived(kind, k):
        slot = peer(k)[0] if kind in (KN, VN) else k
        pltpu.make_async_copy(src(kind, 0), dsts[kind].at[slot], recv_sem.at[kind, k]).wait()

    local(KC).start()
    local(VC).start()
    pl.semaphore_wait(barrier, NDEV - 1)
    order = (1, 2, 4, 6, 3, 5, 7)
    for k in order:
        for kind in (KC, VC):
            remote(kind, k).start()
    acc[...] = jnp.zeros_like(acc)
    l_s[...] = jnp.zeros_like(l_s)
    m_s[...] = jnp.full(m_s.shape, NEG, jnp.float32)
    for cp in loads:
        cp.wait()

    def project(t, n):
        return jnp.dot(x_s[...], wbuf[t % NBUF, :, n * 256:(n + 1) * 256], preferred_element_type=jnp.float32).astype(jnp.bfloat16)

    def rope(rows):
        v = rows.astype(jnp.float32)
        return (v * cos_s[...] + pltpu.roll(v, hd // 2, 1) * sin_s[...]).astype(jnp.bfloat16)

    def q_tile(i, carry):
        @pl.when(i > 0)
        def _():
            for core in range(2):
                kc = i % 4
                remote(QN, 2 * kc + core).start()

        @pl.when(i < 2)
        def _():
            wq_tile(i + 2).start()

        @pl.when(i >= 2)
        def _():
            wk_tile(i - 2).start()

        wq_tile(i).wait()
        chip = q_chip(i)
        for n in range(wide // 256):
            rows = project(i, n)
            for h in range(2):
                head = 2 * n + h
                r = head % group
                q_send[2 * chip + head // group, r * tok:(r + 1) * tok, :] = rope(rows[:, h * hd:(h + 1) * hd])
        return carry

    lax.fori_loop(0, 4, q_tile, 0)

    def k_tile(i, carry):
        wv_tile(i).start()
        wk_tile(i).wait()
        for n in range(2):
            rows = project(4 + i, n)
            for h in range(2):
                k_rows[:, head_cols(4 * i + 2 * n + h)] = rope(rows[:, h * hd:(h + 1) * hd])

        @pl.when(i == 0)
        def _():
            remote(QN, 1).start()
            local(QN).start()
        return carry

    lax.fori_loop(0, 2, k_tile, 0)

    def v_tile(i, carry):
        wv_tile(i).wait()
        for n in range(2):
            v_rows[:, pl.ds(pl.multiple_of(512 * i + 256 * n, 256), 256)] = project(6 + i, n)

        @pl.when(i == 0)
        def _():
            for k in order:
                remote(KN, k).start()
            local(KN).start()
        return carry

    lax.fori_loop(0, 2, v_tile, 0)
    k_out = pltpu.make_async_copy(k_rows, ko_hbm, in_sem.at[0])
    v_out = pltpu.make_async_copy(v_rows, vo_hbm, in_sem.at[1])
    k_out.start()

    def qk(keys, k, r):
        return lax.dot_general(keys, q_s[k, r * tok:(r + 1) * tok, :], (((1,), (1,)), ((), ())), preferred_element_type=jnp.float32)

    def soft_pv(k, r, s, mx, vt):
        cols = slice(r * tok, (r + 1) * tok)
        m_old = m_s[k, :, cols]
        m_new = jnp.maximum(m_old, mx * c2)
        m_s[k, :, cols] = m_new
        alpha = jnp.exp2(m_old - m_new)
        p = jnp.exp2(s * c2 - m_new)
        l_s[k, :, cols] = l_s[k, :, cols] * alpha + jnp.sum(p, axis=0, keepdims=True)
        pv = lax.dot_general(vt, p.astype(jnp.bfloat16), (((1,), (0,)), ((), ())), preferred_element_type=jnp.float32)
        acc[k, :, cols] = acc[k, :, cols] * alpha + pv

    def kchunk(j):
        return kc_s[pl.ds(2 * j, 2)].reshape(2 * tok, hd)

    def cache_chunk(j):
        for core in range(2):
            arrived(KC, 2 * j + core)
            arrived(VC, 2 * j + core)
            vc_t[j, :, core * tok:(core + 1) * tok] = vc_raw[2 * j + core].T

    cache_chunk(0)
    arrived(QN, 0)
    for k in order:
        remote(VN, k).start()
    local(VN).start()
    v_out.start()
    s0 = qk(kchunk(0), 0, 0)
    s_s[0] = s0
    n1 = NDEV * 4

    def phase1(t, mx):
        k, j = t // 4, t % 4
        tn = jnp.minimum(t + 1, n1 - 1)
        kn_, jn_ = tn // 4, tn % 4

        @pl.when(jnp.logical_and(k == 0, j < 3))
        def _():
            cache_chunk(jn_)

        @pl.when(jnp.logical_and(j == 3, k < NDEV - 1))
        def _():
            arrived(QN, kn_)

        for r in range(group):
            nr = (r + 1) % group
            s_next = qk(kchunk(j), k, nr) if nr else qk(kchunk(jn_), kn_, 0)
            cur = s_s[r]
            s_s[nr] = s_next
            soft_pv(k, r, cur, mx, vc_t[j])
            mx = jnp.max(s_next, axis=0, keepdims=True)
        return mx

    lax.fori_loop(0, n1, phase1, jnp.max(s0, axis=0, keepdims=True))

    def new_block(k, carry):
        arrived(KN, k)
        arrived(VN, k)
        dev = peer(k)[0]
        vn_t[dev] = vn_raw[dev].T
        return carry

    lax.fori_loop(0, NDEV, new_block, 0)
    ahead = lax.broadcasted_iota(jnp.int32, (tok, tok), 0) <= lax.broadcasted_iota(jnp.int32, (tok, tok), 1)
    half = pl.ds(0, tok)

    def send_out(k):
        return pltpu.make_async_remote_copy(src_ref=osend.at[k], dst_ref=o_hbm.at[:, group_cols(me)], send_sem=osend_sem.at[k],
                                            recv_sem=orecv_sem.at[k], device_id=peer(k)[1], device_id_type=MESH_ID)

    def phase2(kk, carry):
        k = NDEV - 1 - kk
        p = peer(k)[0]
        s = jnp.where(ahead, qk(kn_s[p], k, 0), NEG)
        s_s[0, half] = s
        mx = jnp.max(s, axis=0, keepdims=True)
        for r in range(group):
            nr = (r + 1) % group
            s_next = jnp.where(ahead, qk(kn_s[p], k, nr), NEG) if nr else qk(kn_s[0], k, 0)
            cur = s_s[r, half]
            s_s[nr, half] = s_next
            soft_pv(k, r, cur, mx, vn_t[p])
            mx = jnp.max(s_next, axis=0, keepdims=True)

        @pl.when(kk > 0)
        def _():
            send_out(k + 1).start()

        def earlier(j, mx):
            jn = jnp.minimum(j + 1, p - 1)
            for r in range(group):
                nr = (r + 1) % group
                s_next = qk(kn_s[j], k, nr) if nr else qk(kn_s[jn], k, 0)
                cur = s_s[r, half]
                s_s[nr, half] = s_next
                soft_pv(k, r, cur, mx, vn_t[j])
                mx = jnp.max(s_next, axis=0, keepdims=True)
            return mx

        lax.fori_loop(0, p, earlier, mx)
        for r in range(group):
            cols = slice(r * tok, (r + 1) * tok)
            o_t = acc[k, :, cols] * (1.0 / l_s[k, :, cols])
            osend[k, :, r * hd:(r + 1) * hd] = o_t.T.astype(jnp.bfloat16)
        return carry

    lax.fori_loop(0, NDEV, phase2, 0)
    own = pltpu.make_async_copy(osend.at[0], o_hbm.at[:, group_cols(me)], orecv_sem.at[0])
    own.start()
    k_out.wait()
    v_out.wait()
    for k in range(1, NDEV):
        for kind in range(5):
            remote(kind, k).wait_send()
        send_out(k).wait_send()
        pltpu.make_async_copy(osend.at[k], o_hbm.at[:, group_cols(peer(k)[0])], orecv_sem.at[k]).wait()
    own.wait()


def layer(x_loc, w_q, w_k, w_v, cos_f, sin_f, kc_t, vc_t):
    kv_heads, tok, hd = kc_t.shape
    d_model = x_loc.shape[1]
    group = w_q.shape[1] // (kv_heads * hd)
    rows = group * tok
    bf, f32 = jnp.bfloat16, jnp.float32
    hbm = pl.BlockSpec(memory_space=pl.ANY)
    sds = jax.ShapeDtypeStruct
    dma = pltpu.SemaphoreType.DMA
    return pl.pallas_call(
        functools.partial(layer_kernel, group, tok, hd ** -0.5),
        out_shape=(sds((tok, kv_heads * group * hd), bf), sds((tok, kv_heads * hd), bf), sds((tok, kv_heads * hd), bf)),
        in_specs=[hbm] * 8,
        out_specs=(hbm, hbm, hbm),
        scratch_shapes=[
            pltpu.VMEM((tok, d_model), bf),
            pltpu.VMEM((tok, hd), f32),
            pltpu.VMEM((tok, hd), f32),
            pltpu.VMEM((NBUF, d_model, 2 * group * hd), bf),
            pltpu.VMEM((NDEV, rows, hd), bf),
            pltpu.VMEM((tok, kv_heads * hd), bf),
            pltpu.VMEM((tok, kv_heads * hd), bf),
            pltpu.VMEM((NDEV, rows, hd), bf),
            pltpu.VMEM((NDEV, tok, hd), bf),
            pltpu.VMEM((NDEV, tok, hd), bf),
            pltpu.VMEM((NDEV // 2, hd, 2 * tok), bf),
            pltpu.VMEM((NDEV, tok, hd), bf),
            pltpu.VMEM((NDEV, tok, hd), bf),
            pltpu.VMEM((NDEV, hd, tok), bf),
            pltpu.VMEM((NDEV, hd, rows), f32),
            pltpu.VMEM((NDEV, 1, rows), f32),
            pltpu.VMEM((NDEV, 1, rows), f32),
            pltpu.VMEM((group, 2 * tok, tok), f32),
            pltpu.VMEM((NDEV, tok, group * hd), bf),
            dma((3,)),
            dma((NBUF,)),
            dma((5, NDEV)),
            dma((5, NDEV)),
            dma((NDEV,)),
            dma((NDEV,)),
        ],
        compiler_params=pltpu.CompilerParams(collective_id=0, has_side_effects=True, vmem_limit_bytes=60 * 2**20),
        name='head_layer',
    )(x_loc, w_q, w_k, w_v, cos_f, sin_f, kc_t, vc_t)


def solution(mesh):
    seq_size = mesh.shape['sp'] * mesh.shape['cp']
    cp_size = mesh.shape['cp']
    row_spec = P(('dp', 'sp', 'cp'))

    def local_fn(x_loc, kc_loc, vc_loc, w_q, w_k, w_v, w_o):
        tok, d_model = x_loc.shape
        cache_loc, kv_heads, hd = kc_loc.shape
        seq_idx = lax.axis_index('sp') * cp_size + lax.axis_index('cp')
        kc_t = jnp.transpose(kc_loc, (1, 0, 2))
        vc_t = jnp.transpose(vc_loc, (1, 0, 2))
        cos_f, sin_f = rope_tables(cache_loc * seq_size + seq_idx * tok + jnp.arange(tok), hd)
        o_rows, k_rows, v_rows = layer(x_loc, w_q, w_k, w_v, cos_f, sin_f, kc_t, vc_t)
        y_loc = jnp.dot(o_rows, w_o, preferred_element_type=jnp.float32).astype(jnp.bfloat16)
        return y_loc, k_rows.reshape(tok, kv_heads, hd), v_rows.reshape(tok, kv_heads, hd)

    return jax.shard_map(local_fn, mesh=mesh, in_specs=(row_spec, row_spec, row_spec, P(), P(), P(), P()), out_specs=(row_spec, row_spec, row_spec), check_vma=False)
```

```python
import functools

import jax
import jax.numpy as jnp
from jax import lax
from jax.experimental import pallas as pl
from jax.experimental.pallas import tpu as pltpu
from jax.sharding import PartitionSpec as P

ROPE_BASE = 500000
MESH_ID = pl.DeviceIdType.MESH
NDEV = 8
NEG = -1e30
LOG2E = 1.4426950408889634
KC, VC, QN, KN, VN = range(5)
NBUF = 4


def rope_tables(positions, head_dim):
    half = jnp.arange(head_dim) % (head_dim // 2)
    inv_freq = 1.0 / (ROPE_BASE ** ((2 * half).astype(jnp.float32) / head_dim))
    angles = positions.astype(jnp.float32)[:, None] * inv_freq[None, :]
    sign = jnp.where(jnp.arange(head_dim) < head_dim // 2, -1.0, 1.0)
    return jnp.cos(angles), jnp.sin(angles) * sign


def layer_kernel(group, tok, scale, x_hbm, wq_hbm, wk_hbm, wv_hbm, wo_hbm, cos_hbm, sin_hbm, kc_hbm, vc_hbm, y_hbm, ko_hbm, vo_hbm,
                 x_s, cos_s, sin_s, wbuf, q_send, k_rows, v_rows, q_s, kc_s, vc_raw, vc_t, kn_s, vn_raw, vn_t, acc, m_s, l_s, s_s, osend, o_s,
                 in_sem, w_sem, send_sem, recv_sem, osend_sem, orecv_sem):
    y = lax.axis_index('sp')
    xc = lax.axis_index('cp')
    x, c = xc // 2, xc % 2
    me = y * 4 + xc
    c2 = scale * LOG2E
    hd = cos_s.shape[1]
    gw = group * hd
    wide = wbuf.shape[2]

    def peer(k):
        py, px, pc = (y + k // 4) % 2, (x + (k // 2) % 2) % 2, (c + k % 2) % 2
        return py * 4 + px * 2 + pc, (0, py, px * 2 + pc)

    def head_cols(dev):
        return pl.ds(pl.multiple_of(dev * hd, hd), hd)

    def group_cols(dev):
        return pl.ds(pl.multiple_of(dev * gw, gw), gw)

    barrier = pltpu.get_barrier_semaphore()
    for k in range(1, NDEV):
        pl.semaphore_signal(barrier, inc=1, device_id=peer(k)[1], device_id_type=MESH_ID)

    def q_chip(i):
        kc = (i + 1) % 4
        return ((y + kc // 2) % 2) * 2 + (x + kc % 2) % 2

    def w_copy(w_hbm, col, width, t):
        return pltpu.make_async_copy(w_hbm.at[:, pl.ds(pl.multiple_of(col, 256), width)], wbuf.at[t % NBUF, :, pl.ds(0, width)], w_sem.at[t % NBUF])

    def wq_tile(i):
        return w_copy(wq_hbm, q_chip(i) * wide, wide, i)

    def wk_tile(i):
        return w_copy(wk_hbm, i * 512, 512, 4 + i)

    def wv_tile(i):
        return w_copy(wv_hbm, i * 512, 512, 6 + i)

    def wo_tile(n):
        return w_copy(wo_hbm, n * wide, wide, n)

    loads = [pltpu.make_async_copy(x_hbm, x_s, in_sem.at[0]), pltpu.make_async_copy(cos_hbm, cos_s, in_sem.at[1]), pltpu.make_async_copy(sin_hbm, sin_s, in_sem.at[2])]
    loads[0].start()
    wq_tile(0).start()
    loads[1].start()
    loads[2].start()
    wq_tile(1).start()

    def src(kind, dev):
        if kind in (KN, VN):
            return (k_rows if kind == KN else v_rows).at[:, head_cols(dev)]
        return {KC: kc_hbm, VC: vc_hbm, QN: q_send}[kind].at[dev]

    dsts = (kc_s, vc_raw, q_s, kn_s, vn_raw)

    def local(kind):
        slot = me if kind in (KN, VN) else 0
        return pltpu.make_async_copy(src(kind, me), dsts[kind].at[slot], recv_sem.at[kind, 0])

    def remote(kind, k):
        p, did = peer(k)
        slot = me if kind in (KN, VN) else k
        return pltpu.make_async_remote_copy(src_ref=src(kind, p), dst_ref=dsts[kind].at[slot], send_sem=send_sem.at[kind, k],
                                            recv_sem=recv_sem.at[kind, k], device_id=did, device_id_type=MESH_ID)

    def arrived(kind, k):
        slot = peer(k)[0] if kind in (KN, VN) else k
        pltpu.make_async_copy(src(kind, 0), dsts[kind].at[slot], recv_sem.at[kind, k]).wait()

    local(KC).start()
    local(VC).start()
    pl.semaphore_wait(barrier, NDEV - 1)
    order = (1, 2, 4, 6, 3, 5, 7)
    for k in order:
        for kind in (KC, VC):
            remote(kind, k).start()
    acc[...] = jnp.zeros_like(acc)
    l_s[...] = jnp.zeros_like(l_s)
    m_s[...] = jnp.full(m_s.shape, NEG, jnp.float32)
    for cp in loads:
        cp.wait()

    def project(t, n):
        return jnp.dot(x_s[...], wbuf[t % NBUF, :, n * 256:(n + 1) * 256], preferred_element_type=jnp.float32).astype(jnp.bfloat16)

    def rope(rows):
        v = rows.astype(jnp.float32)
        return v * cos_s[...] + pltpu.roll(v, hd // 2, 1) * sin_s[...]

    def q_tile(i, carry):
        @pl.when(jnp.logical_and(i > 0, i < 3))
        def _():
            for core in range(2):
                remote(QN, 2 * i + core).start()

        @pl.when(i < 2)
        def _():
            wq_tile(i + 2).start()

        @pl.when(i >= 2)
        def _():
            wk_tile(i - 2).start()

        wq_tile(i).wait()
        chip = q_chip(i)
        for n in range(wide // 256):
            rows = project(i, n)
            for h in range(2):
                head = 2 * n + h
                r = head % group
                q_send[2 * chip + head // group, r * tok:(r + 1) * tok, :] = (rope(rows[:, h * hd:(h + 1) * hd]) * c2).astype(jnp.bfloat16)
        return carry

    lax.fori_loop(0, 4, q_tile, 0)

    def k_tile(i, carry):
        wv_tile(i).start()
        wk_tile(i).wait()
        for n in range(2):
            rows = project(4 + i, n)
            for h in range(2):
                k_rows[:, head_cols(4 * i + 2 * n + h)] = rope(rows[:, h * hd:(h + 1) * hd]).astype(jnp.bfloat16)

        @pl.when(i == 0)
        def _():
            remote(QN, 1).start()
            local(QN).start()
        return carry

    lax.fori_loop(0, 2, k_tile, 0)

    def v_tile(i, carry):
        wv_tile(i).wait()
        for n in range(2):
            v_rows[:, pl.ds(pl.multiple_of(512 * i + 256 * n, 256), 256)] = project(6 + i, n)

        @pl.when(i == 0)
        def _():
            for k in order:
                remote(KN, k).start()
            local(KN).start()
        return carry

    lax.fori_loop(0, 2, v_tile, 0)
    k_out = pltpu.make_async_copy(k_rows, ko_hbm, in_sem.at[0])
    v_out = pltpu.make_async_copy(v_rows, vo_hbm, in_sem.at[1])
    k_out.start()

    def qk(keys, k, r):
        return lax.dot_general(keys, q_s[k, r * tok:(r + 1) * tok, :], (((1,), (1,)), ((), ())), preferred_element_type=jnp.float32)

    def soft_pv(k, r, s, mx, vt):
        cols = slice(r * tok, (r + 1) * tok)
        m_old = m_s[k, :, cols]
        m_new = jnp.maximum(m_old, mx)
        m_s[k, :, cols] = m_new
        alpha = jnp.exp2(m_old - m_new)
        p = jnp.exp2(s - m_new)
        l_s[k, :, cols] = l_s[k, :, cols] * alpha + jnp.sum(p, axis=0, keepdims=True)
        pv = lax.dot_general(vt, p.astype(jnp.bfloat16), (((1,), (0,)), ((), ())), preferred_element_type=jnp.float32)
        acc[k, :, cols] = acc[k, :, cols] * alpha + pv

    def kchunk(j):
        return kc_s[pl.ds(2 * j, 2)].reshape(2 * tok, hd)

    def cache_chunk(j):
        for core in range(2):
            arrived(KC, 2 * j + core)
            arrived(VC, 2 * j + core)
            vc_t[j, :, core * tok:(core + 1) * tok] = vc_raw[2 * j + core].T

    for n in range(4):
        wo_tile(n).start()
    cache_chunk(0)
    arrived(QN, 0)
    for k in order:
        remote(VN, k).start()
    for k in (6, 7):
        remote(QN, k).start()
    local(VN).start()
    v_out.start()
    def cache_part(first, count, waits):
        s0 = qk(kchunk(0), first, 0)
        s_s[0] = s0
        steps = 4 * count

        def step(t, mx):
            k, j = first + t // 4, t % 4
            tn = jnp.minimum(t + 1, steps - 1)
            k_next, j_next = first + tn // 4, tn % 4
            if waits:
                @pl.when(t < 3)
                def _():
                    cache_chunk(j_next)

                @pl.when(jnp.logical_and(j == 3, t < steps - 1))
                def _():
                    arrived(QN, k_next)

            for r in range(group):
                nr = (r + 1) % group
                s_next = qk(kchunk(j), k, nr) if nr else qk(kchunk(j_next), k_next, 0)
                cur = s_s[r]
                s_s[nr] = s_next
                soft_pv(k, r, cur, mx, vc_t[j])
                mx = jnp.max(s_next, axis=0, keepdims=True)
            return mx

        lax.fori_loop(0, steps, step, jnp.max(s0, axis=0, keepdims=True))

    cache_part(0, 6, True)

    def new_block(k, carry):
        arrived(KN, k)
        arrived(VN, k)
        dev = peer(k)[0]
        vn_t[dev] = vn_raw[dev].T
        return carry

    lax.fori_loop(0, NDEV, new_block, 0)
    ahead = lax.broadcasted_iota(jnp.int32, (tok, tok), 0) <= lax.broadcasted_iota(jnp.int32, (tok, tok), 1)
    half = pl.ds(0, tok)

    def send_out(k):
        return pltpu.make_async_remote_copy(src_ref=osend.at[k], dst_ref=o_s.at[k // 2, :, group_cols(c)], send_sem=osend_sem.at[k],
                                            recv_sem=orecv_sem.at[k], device_id=peer(k)[1], device_id_type=MESH_ID)

    def out_arrived(k):
        pltpu.make_async_copy(osend.at[k], o_s.at[k // 2, :, group_cols(peer(k)[0] % 2)], orecv_sem.at[k]).wait()

    def item(i):
        return i + 2 - (i // 6) * (2 * i - 5)

    def phase2(i, carry):
        k = item(i)
        p = peer(k)[0]

        @pl.when(i // 2 == 2)
        def _():
            arrived(QN, k)
            cache_part(k, 1, False)

        s = jnp.where(ahead, qk(kn_s[p], k, 0), NEG)
        s_s[0, half] = s
        mx = jnp.max(s, axis=0, keepdims=True)
        for r in range(group):
            nr = (r + 1) % group
            s_next = jnp.where(ahead, qk(kn_s[p], k, nr), NEG) if nr else qk(kn_s[0], k, 0)
            cur = s_s[r, half]
            s_s[nr, half] = s_next
            soft_pv(k, r, cur, mx, vn_t[p])
            mx = jnp.max(s_next, axis=0, keepdims=True)

        @pl.when(i > 0)
        def _():
            send_out(item(i - 1)).start()

        def earlier(j, mx):
            jn = jnp.minimum(j + 1, p - 1)
            for r in range(group):
                nr = (r + 1) % group
                s_next = qk(kn_s[j], k, nr) if nr else qk(kn_s[jn], k, 0)
                cur = s_s[r, half]
                s_s[nr, half] = s_next
                soft_pv(k, r, cur, mx, vn_t[j])
                mx = jnp.max(s_next, axis=0, keepdims=True)
            return mx

        lax.fori_loop(0, p, earlier, mx)
        for r in range(group):
            cols = slice(r * tok, (r + 1) * tok)
            o_t = acc[k, :, cols] * (1.0 / l_s[k, :, cols])
            osend[k, :, r * hd:(r + 1) * hd] = o_t.T.astype(jnp.bfloat16)
        return carry

    lax.fori_loop(0, NDEV, phase2, 0)

    own = pltpu.make_async_copy(osend.at[0], o_s.at[0, :, group_cols(c)], orecv_sem.at[0])
    for n in range(4):
        wo_tile(n).wait()
    k_out.wait()
    v_out.wait()
    quarter = tok // 4

    def y_piece(kc, old, last):
        chip = ((y + kc // 2) % 2) * 2 + (x + kc % 2) % 2
        w_rows = pl.ds(pl.multiple_of(chip * wide, wide), wide)

        def tiles(n, carry):
            for sub in range(3):
                val = jnp.dot(o_s[kc], wbuf[n, w_rows, sub * 256:(sub + 1) * 256], preferred_element_type=jnp.float32)
                if old:
                    val = val + jnp.concatenate([acc[2 * n + (4 * sub + u) // 6, :, (4 * sub + u) % 6 * 256:(4 * sub + u) % 6 * 256 + 256] for u in range(4)], axis=0)
                if last:
                    x_s[:, pl.ds(pl.multiple_of(n * wide + sub * 256, 256), 256)] = val.astype(jnp.bfloat16)
                else:
                    for u in range(4):
                        f = 4 * sub + u
                        acc[2 * n + f // 6, :, f % 6 * 256:f % 6 * 256 + 256] = val[u * quarter:(u + 1) * quarter]
            if last:
                @pl.when(n > 0)
                def _():
                    y_copy(n - 1).start()
            return carry

        lax.fori_loop(0, 4, tiles, 0)

    def y_copy(n):
        cols = pl.ds(pl.multiple_of(n * wide, wide), wide)
        return pltpu.make_async_copy(x_s.at[:, cols], y_hbm.at[:, cols], w_sem.at[n])

    out_arrived(2)
    out_arrived(3)
    y_piece(1, False, False)
    own.start()
    out_arrived(4)
    out_arrived(5)
    y_piece(2, True, False)
    out_arrived(1)
    own.wait()
    y_piece(0, True, False)
    out_arrived(6)
    out_arrived(7)
    y_piece(3, True, True)
    for k in range(1, NDEV):
        for kind in range(5):
            remote(kind, k).wait_send()
        send_out(k).wait_send()
    y_copy(3).start()
    for n in range(4):
        y_copy(n).wait()


def layer(x_loc, w_q, w_k, w_v, w_o, cos_f, sin_f, kc_t, vc_t):
    kv_heads, tok, hd = kc_t.shape
    d_model = x_loc.shape[1]
    group = w_q.shape[1] // (kv_heads * hd)
    rows = group * tok
    bf, f32 = jnp.bfloat16, jnp.float32
    hbm = pl.BlockSpec(memory_space=pl.ANY)
    sds = jax.ShapeDtypeStruct
    dma = pltpu.SemaphoreType.DMA
    return pl.pallas_call(
        functools.partial(layer_kernel, group, tok, hd ** -0.5),
        out_shape=(sds((tok, d_model), bf), sds((tok, kv_heads * hd), bf), sds((tok, kv_heads * hd), bf)),
        in_specs=[hbm] * 9,
        out_specs=(hbm, hbm, hbm),
        scratch_shapes=[
            pltpu.VMEM((tok, d_model), bf),
            pltpu.VMEM((tok, hd), f32),
            pltpu.VMEM((tok, hd), f32),
            pltpu.VMEM((NBUF, d_model, 2 * group * hd), bf),
            pltpu.VMEM((NDEV, rows, hd), bf),
            pltpu.VMEM((tok, kv_heads * hd), bf),
            pltpu.VMEM((tok, kv_heads * hd), bf),
            pltpu.VMEM((NDEV, rows, hd), bf),
            pltpu.VMEM((NDEV, tok, hd), bf),
            pltpu.VMEM((NDEV, tok, hd), bf),
            pltpu.VMEM((NDEV // 2, hd, 2 * tok), bf),
            pltpu.VMEM((NDEV, tok, hd), bf),
            pltpu.VMEM((NDEV, tok, hd), bf),
            pltpu.VMEM((NDEV, hd, tok), bf),
            pltpu.VMEM((NDEV, hd, rows), f32),
            pltpu.VMEM((NDEV, 1, rows), f32),
            pltpu.VMEM((NDEV, 1, rows), f32),
            pltpu.VMEM((group, 2 * tok, tok), f32),
            pltpu.VMEM((NDEV, tok, group * hd), bf),
            pltpu.VMEM((NDEV // 2, tok, 2 * group * hd), bf),
            dma((3,)),
            dma((NBUF,)),
            dma((5, NDEV)),
            dma((5, NDEV)),
            dma((NDEV,)),
            dma((NDEV,)),
        ],
        compiler_params=pltpu.CompilerParams(collective_id=0, has_side_effects=True, vmem_limit_bytes=63 * 2**20),
        name='head_layer',
    )(x_loc, w_q, w_k, w_v, w_o, cos_f, sin_f, kc_t, vc_t)


def solution(mesh):
    seq_size = mesh.shape['sp'] * mesh.shape['cp']
    cp_size = mesh.shape['cp']
    row_spec = P(('dp', 'sp', 'cp'))

    def local_fn(x_loc, kc_loc, vc_loc, w_q, w_k, w_v, w_o):
        tok, d_model = x_loc.shape
        cache_loc, kv_heads, hd = kc_loc.shape
        seq_idx = lax.axis_index('sp') * cp_size + lax.axis_index('cp')
        kc_t = jnp.transpose(kc_loc, (1, 0, 2))
        vc_t = jnp.transpose(vc_loc, (1, 0, 2))
        cos_f, sin_f = rope_tables(cache_loc * seq_size + seq_idx * tok + jnp.arange(tok), hd)
        y_loc, k_rows, v_rows = layer(x_loc, w_q, w_k, w_v, w_o, cos_f, sin_f, kc_t, vc_t)
        return y_loc, k_rows.reshape(tok, kv_heads, hd), v_rows.reshape(tok, kv_heads, hd)

    return jax.shard_map(local_fn, mesh=mesh, in_specs=(row_spec, row_spec, row_spec, P(), P(), P(), P()), out_specs=(row_spec, row_spec, row_spec), check_vma=False)
```

```python
import functools

import jax
import jax.numpy as jnp
import numpy as np
from jax import lax
from jax.experimental import pallas as pl
from jax.experimental.pallas import tpu as pltpu
from jax.sharding import PartitionSpec as P

ROPE_BASE = 500000
MESH_ID = pl.DeviceIdType.MESH
NDEV = 8
NEG = -1e30
LOG2E = 1.4426950408889634
KC, VC, QN, KN, VN = range(5)
NBUF = 4


def rope_table(first, count, head_dim):
    f32 = np.float32
    inv_freq = f32(1.0) / (f32(ROPE_BASE) ** (np.arange(0, head_dim, 2, dtype=f32) / f32(head_dim)))
    angles = (first + np.arange(count)).astype(f32)[:, None] * inv_freq[None, :]
    return np.concatenate([np.cos(angles.astype(np.float64)), np.sin(angles.astype(np.float64))], axis=1).astype(f32)


def layer_kernel(group, tok, scale, x_hbm, wq_hbm, wk_hbm, wv_hbm, wo_hbm, table_hbm, kc_hbm, vc_hbm, y_hbm, ko_hbm, vo_hbm,
                 x_s, cos_s, sin_s, wbuf, q_send, k_rows, v_rows, q_s, kc_s, vc_raw, vc_t, kn_s, vn_raw, vn_t, acc, m_s, l_s, s_s, osend, o_s, kc_out, vc_out,
                 in_sem, w_sem, send_sem, recv_sem, osend_sem, orecv_sem):
    y = lax.axis_index('sp')
    xc = lax.axis_index('cp')
    x, c = xc // 2, xc % 2
    me = y * 4 + xc
    c2 = scale * LOG2E
    hd = cos_s.shape[1]
    gw = group * hd
    wide = wbuf.shape[2]

    def peer(k):
        py, px, pc = (y + k // 4) % 2, (x + (k // 2) % 2) % 2, (c + k % 2) % 2
        return py * 4 + px * 2 + pc, (0, py, px * 2 + pc)

    def head_cols(dev):
        return pl.ds(pl.multiple_of(dev * hd, hd), hd)

    def group_cols(dev):
        return pl.ds(pl.multiple_of(dev * gw, gw), gw)

    barrier = pltpu.get_barrier_semaphore()
    for k in range(1, NDEV):
        pl.semaphore_signal(barrier, inc=1, device_id=peer(k)[1], device_id_type=MESH_ID)

    def q_chip(i):
        kc = (i + 1) % 4
        return ((y + kc // 2) % 2) * 2 + (x + kc % 2) % 2

    def w_copy(w_hbm, col, width, t):
        return pltpu.make_async_copy(w_hbm.at[:, pl.ds(pl.multiple_of(col, 256), width)], wbuf.at[t % NBUF, :, pl.ds(0, width)], w_sem.at[t % NBUF])

    def wq_tile(i):
        return w_copy(wq_hbm, q_chip(i) * wide, wide, i)

    def wk_tile(i):
        return w_copy(wk_hbm, i * 512, 512, 4 + i)

    def wv_tile(i):
        return w_copy(wv_hbm, i * 512, 512, 6 + i)

    def wo_tile(n):
        return w_copy(wo_hbm, n * wide, wide, n)

    loads = [pltpu.make_async_copy(x_hbm, x_s, in_sem.at[0]), pltpu.make_async_copy(table_hbm.at[pl.ds(pl.multiple_of(me * tok, tok), tok)], cos_s, in_sem.at[1])]
    raw = [pltpu.make_async_copy(hbm, osend.at[:, :, pl.ds(n * hd, hd)], in_sem.at[2 + n]) for n, hbm in enumerate((kc_hbm, vc_hbm))]
    for cp in raw + loads:
        cp.start()
    wq_tile(0).start()
    wq_tile(1).start()

    def src(kind, dev):
        if kind in (KN, VN):
            return (k_rows if kind == KN else v_rows).at[:, head_cols(dev)]
        return {KC: kc_out, VC: vc_out, QN: q_send}[kind].at[dev]

    dsts = (kc_s, vc_raw, q_s, kn_s, vn_raw)

    def local(kind):
        slot = me if kind in (KN, VN) else 0
        return pltpu.make_async_copy(src(kind, me), dsts[kind].at[slot], recv_sem.at[kind, 0])

    def remote(kind, k):
        p, did = peer(k)
        slot = me if kind in (KN, VN) else k
        return pltpu.make_async_remote_copy(src_ref=src(kind, p), dst_ref=dsts[kind].at[slot], send_sem=send_sem.at[kind, k],
                                            recv_sem=recv_sem.at[kind, k], device_id=did, device_id_type=MESH_ID)

    def arrived(kind, k):
        slot = peer(k)[0] if kind in (KN, VN) else k
        pltpu.make_async_copy(src(kind, 0), dsts[kind].at[slot], recv_sem.at[kind, k]).wait()

    for n, out in enumerate((kc_out, vc_out)):
        raw[n].wait()
        for b in range(NDEV):
            s_s[n, b // 4, b % 4 * tok:(b % 4 + 1) * tok, :] = osend[b, :, n * hd:(n + 1) * hd].astype(jnp.float32)
        for h in range(NDEV):
            for g in range(2):
                out[h, g * tok // 2:(g + 1) * tok // 2, :] = s_s[n, g, pl.ds(h, tok // 2, stride=NDEV), :].astype(jnp.bfloat16)
    pl.semaphore_wait(barrier, NDEV - 1)
    local(KC).start()
    local(VC).start()
    order = (1, 2, 4, 6, 3, 5, 7)
    for k in order:
        for kind in (KC, VC):
            remote(kind, k).start()
    acc[...] = jnp.zeros_like(acc)
    l_s[...] = jnp.zeros_like(l_s)
    m_s[...] = jnp.full(m_s.shape, NEG, jnp.float32)
    for cp in loads:
        cp.wait()
    table = cos_s[...]
    turned = pltpu.roll(table, hd // 2, 1)
    low = lax.broadcasted_iota(jnp.int32, table.shape, 1) < hd // 2
    cos_s[...] = jnp.where(low, table, turned)
    sin_s[...] = jnp.where(low, -turned, table)

    def project(t, n):
        return jnp.dot(x_s[...], wbuf[t % NBUF, :, n * 256:(n + 1) * 256], preferred_element_type=jnp.float32).astype(jnp.bfloat16)

    def rope(rows):
        v = rows.astype(jnp.float32)
        return v * cos_s[...] + pltpu.roll(v, hd // 2, 1) * sin_s[...]

    def q_tile(i, carry):
        @pl.when(jnp.logical_and(i > 0, i < 3))
        def _():
            for core in range(2):
                remote(QN, 2 * i + core).start()

        @pl.when(i < 2)
        def _():
            wq_tile(i + 2).start()

        @pl.when(i >= 2)
        def _():
            wk_tile(i - 2).start()

        wq_tile(i).wait()
        chip = q_chip(i)
        for n in range(wide // 256):
            rows = project(i, n)
            for h in range(2):
                head = 2 * n + h
                r = head % group
                q_send[2 * chip + head // group, r * tok:(r + 1) * tok, :] = (rope(rows[:, h * hd:(h + 1) * hd]) * c2).astype(jnp.bfloat16)
        return carry

    lax.fori_loop(0, 4, q_tile, 0)

    def k_tile(i, carry):
        wv_tile(i).start()
        wk_tile(i).wait()
        for n in range(2):
            rows = project(4 + i, n)
            for h in range(2):
                k_rows[:, head_cols(4 * i + 2 * n + h)] = rope(rows[:, h * hd:(h + 1) * hd]).astype(jnp.bfloat16)

        @pl.when(i == 0)
        def _():
            remote(QN, 1).start()
            local(QN).start()
        return carry

    lax.fori_loop(0, 2, k_tile, 0)

    def v_tile(i, carry):
        wv_tile(i).wait()
        for n in range(2):
            v_rows[:, pl.ds(pl.multiple_of(512 * i + 256 * n, 256), 256)] = project(6 + i, n)

        @pl.when(i == 0)
        def _():
            for k in order:
                remote(KN, k).start()
            local(KN).start()
        return carry

    lax.fori_loop(0, 2, v_tile, 0)
    news = [pltpu.make_async_copy(osend.at[:, :, pl.ds(n * hd, hd)], hbm, in_sem.at[2 + n]) for n, hbm in enumerate((ko_hbm, vo_hbm))]
    for n, rows in enumerate((k_rows, v_rows)):
        for h in range(NDEV):
            for g in range(2):
                s_s[n, g, pl.ds(h, tok // 2, stride=NDEV), :] = rows[g * tok // 2:(g + 1) * tok // 2, h * hd:(h + 1) * hd].astype(jnp.float32)
        for b in range(NDEV):
            osend[b, :, n * hd:(n + 1) * hd] = s_s[n, b // 4, b % 4 * tok:(b % 4 + 1) * tok, :].astype(jnp.bfloat16)

    for n in range(4):
        wo_tile(n).start()
    for k in order:
        remote(VN, k).start()
    for k in (6, 7):
        remote(QN, k).start()
    local(VN).start()
    for cp in news:
        cp.start()
    def qk(keys, k, rows):
        return lax.dot_general(keys, q_s[k, rows, :], (((1,), (1,)), ((), ())), preferred_element_type=jnp.float32)

    def slab(u, j, rows, cols):
        return j % 2, pl.ds((u * (cols // 256) + j // 2) * rows, rows)

    def put(slot, u, val):
        rows, cols = val.shape
        for j in range(cols // 128):
            side, where = slab(u, j, rows, cols)
            s_s[slot, side, where, :] = val[:, j * 128:(j + 1) * 128]

    def get(slot, u, rows, cols):
        parts = []
        for j in range(cols // 128):
            side, where = slab(u, j, rows, cols)
            parts.append(s_s[slot, side, where, :])
        return jnp.concatenate(parts, axis=1)

    def tile_max(old, val):
        top = jnp.max(val, axis=0, keepdims=True)
        return top if old is None else jnp.maximum(old, top)

    def sub_step(slot, k, cols, size, mx, pieces, depth, vt, following):
        m_old = m_s[k, :, cols]
        m_new = jnp.maximum(m_old, mx)
        m_s[k, :, cols] = m_new
        alpha = jnp.exp2(m_old - m_new)
        total, pv, mx_next = None, None, None
        for u in range(pieces):
            s_next = None if following is None else following(u)
            p = jnp.exp2(get(slot, u, depth, size) - m_new)
            if s_next is not None:
                put(1 - slot, u, s_next)
                mx_next = tile_max(mx_next, s_next)
            part = jnp.sum(p, axis=0, keepdims=True)
            prod = jnp.dot(vt(u), p.astype(jnp.bfloat16), preferred_element_type=jnp.float32)
            total = part if total is None else total + part
            pv = prod if pv is None else pv + prod
        l_s[k, :, cols] = l_s[k, :, cols] * alpha + total
        acc[k, :, cols] = acc[k, :, cols] * alpha + pv
        return mx_next

    def first_tile(pieces, scores):
        mx = None
        for u in range(pieces):
            val = scores(u)
            put(0, u, val)
            mx = tile_max(mx, val)
        return mx

    def cache_chunk(j):
        for core in range(2):
            arrived(KC, 2 * j + core)
            arrived(VC, 2 * j + core)
            vc_t[j, :, core * tok:(core + 1) * tok] = vc_raw[2 * j + core].T

    def cache_part(first, count):
        pieces = NDEV // 2
        steps = 2 * count
        mx0 = first_tile(pieces, lambda u: qk(kc_s[u], first, pl.ds(0, 256)))

        def step(t, mx):
            k, half = first + t // 2, t % 2
            tn = jnp.minimum(t + 1, steps - 1)
            k_next, half_next = first + tn // 2, tn % 2
            tiles = group * tok // 256
            for r in range(tiles):
                if r + 1 < tiles:
                    following = lambda u, r=r: qk(kc_s[pieces * half + u], k, pl.ds((r + 1) * 256, 256))
                else:
                    @pl.when(jnp.logical_and(first == 0, t == 0))
                    def _():
                        cache_chunk(2)
                        cache_chunk(3)

                    @pl.when(jnp.logical_and(half == 1, t < steps - 1))
                    def _():
                        arrived(QN, k_next)

                    following = lambda u: qk(kc_s[pieces * half_next + u], k_next, pl.ds(0, 256))
                mx = sub_step(r % 2, k, pl.ds(r * 256, 256), 256, mx, pieces, tok,
                              lambda u: vc_t[2 * half + u // 2, :, (u % 2) * tok:(u % 2 + 1) * tok], following)
            return mx

        lax.fori_loop(0, steps, step, mx0)

    wide_rows = group * tok // 2

    def causal(h, val):
        key = lax.broadcasted_iota(jnp.int32, (tok, wide_rows), 0)
        row = (lax.broadcasted_iota(jnp.int32, (tok, wide_rows), 1) + h * wide_rows) & (tok - 1)
        return jnp.where(key <= row, val, NEG)

    def row_half(h):
        return pl.ds(h * wide_rows, wide_rows)

    def new_block(k, carry):
        arrived(KN, k)
        arrived(VN, k)
        dev = peer(k)[0]
        vn_t[dev] = vn_raw[dev].T
        return carry

    def send_out(k):
        return pltpu.make_async_remote_copy(src_ref=osend.at[k], dst_ref=o_s.at[k // 2, :, group_cols(c)], send_sem=osend_sem.at[k],
                                            recv_sem=orecv_sem.at[k], device_id=peer(k)[1], device_id_type=MESH_ID)

    def out_arrived(k):
        pltpu.make_async_copy(osend.at[k], o_s.at[k // 2, :, group_cols(peer(k)[0] % 2)], orecv_sem.at[k]).wait()

    def item(i):
        return i + 2 - (i // 6) * (2 * i - 5)

    def new_part(i, carry):
        k = item(i)
        p = peer(k)[0]

        @pl.when(jnp.logical_or(i == 0, i // 2 == 2))
        def _():
            @pl.when(i > 0)
            def _():
                arrived(QN, k)

            cache_part((i // 4) * k, jnp.where(i == 0, 6, 1))

        @pl.when(i == 0)
        def _():
            for cp in news:
                cp.wait()
            lax.fori_loop(0, NDEV, new_block, 0)

        mx = first_tile(1, lambda u: causal(0, qk(kn_s[p], k, row_half(0))))
        mx = sub_step(0, k, row_half(0), wide_rows, mx, 1, tok, lambda u: vn_t[p], lambda u: causal(1, qk(kn_s[p], k, row_half(1))))
        mx = sub_step(1, k, row_half(1), wide_rows, mx, 1, tok, lambda u: vn_t[p], lambda u: qk(kn_s[0], k, row_half(0)))

        @pl.when(i > 0)
        def _():
            send_out(item(i - 1)).start()

        def earlier(j, mx):
            jn = jnp.minimum(j + 1, p - 1)
            mx = sub_step(0, k, row_half(0), wide_rows, mx, 1, tok, lambda u: vn_t[j], lambda u: qk(kn_s[j], k, row_half(1)))
            return sub_step(1, k, row_half(1), wide_rows, mx, 1, tok, lambda u: vn_t[j], lambda u: qk(kn_s[jn], k, row_half(0)))

        lax.fori_loop(0, p, earlier, mx)
        for r in range(group):
            cols = slice(r * tok, (r + 1) * tok)
            o_t = acc[k, :, cols] * (1.0 / l_s[k, :, cols])
            osend[k, :, r * hd:(r + 1) * hd] = o_t.T.astype(jnp.bfloat16)
        return carry

    arrived(QN, 0)
    cache_chunk(0)
    cache_chunk(1)
    lax.fori_loop(0, NDEV, new_part, 0)

    own = pltpu.make_async_copy(osend.at[0], o_s.at[0, :, group_cols(c)], orecv_sem.at[0])
    for n in range(4):
        wo_tile(n).wait()
    quarter = tok // 4

    def y_piece(kc, old, last):
        chip = ((y + kc // 2) % 2) * 2 + (x + kc % 2) % 2
        w_rows = pl.ds(pl.multiple_of(chip * wide, wide), wide)

        def tiles(n, carry):
            for sub in range(3):
                val = jnp.dot(o_s[kc], wbuf[n, w_rows, sub * 256:(sub + 1) * 256], preferred_element_type=jnp.float32)
                if old:
                    val = val + jnp.concatenate([acc[2 * n + (4 * sub + u) // 6, :, (4 * sub + u) % 6 * 256:(4 * sub + u) % 6 * 256 + 256] for u in range(4)], axis=0)
                if last:
                    x_s[:, pl.ds(pl.multiple_of(n * wide + sub * 256, 256), 256)] = val.astype(jnp.bfloat16)
                else:
                    for u in range(4):
                        f = 4 * sub + u
                        acc[2 * n + f // 6, :, f % 6 * 256:f % 6 * 256 + 256] = val[u * quarter:(u + 1) * quarter]
            if last:
                @pl.when(n > 0)
                def _():
                    y_copy(n - 1).start()
            return carry

        lax.fori_loop(0, 4, tiles, 0)

    def y_copy(n):
        cols = pl.ds(pl.multiple_of(n * wide, wide), wide)
        return pltpu.make_async_copy(x_s.at[:, cols], y_hbm.at[:, cols], w_sem.at[n])

    out_arrived(2)
    out_arrived(3)
    y_piece(1, False, False)
    own.start()
    out_arrived(4)
    out_arrived(5)
    y_piece(2, True, False)
    out_arrived(1)
    own.wait()
    y_piece(0, True, False)
    out_arrived(6)
    out_arrived(7)
    y_piece(3, True, True)
    for k in range(1, NDEV):
        for kind in range(5):
            remote(kind, k).wait_send()
        send_out(k).wait_send()
    y_copy(3).start()
    for n in range(4):
        y_copy(n).wait()


def layer(x_loc, w_q, w_k, w_v, w_o, table, kc_loc, vc_loc):
    tok, kv_heads, hd = kc_loc.shape
    d_model = x_loc.shape[1]
    group = w_q.shape[1] // (kv_heads * hd)
    rows = group * tok
    bf, f32 = jnp.bfloat16, jnp.float32
    hbm = pl.BlockSpec(memory_space=pl.ANY)
    sds = jax.ShapeDtypeStruct
    dma = pltpu.SemaphoreType.DMA
    return pl.pallas_call(
        functools.partial(layer_kernel, group, tok, hd ** -0.5),
        out_shape=(sds((tok, d_model), bf), sds((kv_heads, tok, hd), bf), sds((kv_heads, tok, hd), bf)),
        in_specs=[hbm] * 8,
        out_specs=(hbm, hbm, hbm),
        scratch_shapes=[
            pltpu.VMEM((tok, d_model), bf),
            pltpu.VMEM((tok, hd), f32),
            pltpu.VMEM((tok, hd), f32),
            pltpu.VMEM((NBUF, d_model, 2 * group * hd), bf),
            pltpu.VMEM((NDEV, rows, hd), bf),
            pltpu.VMEM((tok, kv_heads * hd), bf),
            pltpu.VMEM((tok, kv_heads * hd), bf),
            pltpu.VMEM((NDEV, rows, hd), bf),
            pltpu.VMEM((NDEV, tok, hd), bf),
            pltpu.VMEM((NDEV, tok, hd), bf),
            pltpu.VMEM((NDEV // 2, hd, 2 * tok), bf),
            pltpu.VMEM((NDEV, tok, hd), bf),
            pltpu.VMEM((NDEV, tok, hd), bf),
            pltpu.VMEM((NDEV, hd, tok), bf),
            pltpu.VMEM((NDEV, hd, rows), f32),
            pltpu.VMEM((NDEV, 1, rows), f32),
            pltpu.VMEM((NDEV, 1, rows), f32),
            pltpu.VMEM((2, 2, 4 * tok, 128), f32),
            pltpu.VMEM((NDEV, tok, group * hd), bf),
            pltpu.VMEM((NDEV // 2, tok, 2 * group * hd), bf),
            pltpu.VMEM((NDEV, tok, hd), bf),
            pltpu.VMEM((NDEV, tok, hd), bf),
            dma((4,)),
            dma((NBUF,)),
            dma((5, NDEV)),
            dma((5, NDEV)),
            dma((NDEV,)),
            dma((NDEV,)),
        ],
        compiler_params=pltpu.CompilerParams(collective_id=0, has_side_effects=True, vmem_limit_bytes=63 * 2**20),
        name='head_layer',
    )(x_loc, w_q, w_k, w_v, w_o, table, kc_loc.reshape(kv_heads, tok, hd), vc_loc.reshape(kv_heads, tok, hd))


def solution(mesh):
    seq_size = mesh.shape['sp'] * mesh.shape['cp']
    row_spec = P(('dp', 'sp', 'cp'))

    def local_fn(x_loc, kc_loc, vc_loc, w_q, w_k, w_v, w_o):
        tok, d_model = x_loc.shape
        cache_loc, kv_heads, hd = kc_loc.shape
        table = jnp.asarray(rope_table(cache_loc * seq_size, tok * seq_size, hd))
        y_loc, k_rows, v_rows = layer(x_loc, w_q, w_k, w_v, w_o, table, kc_loc, vc_loc)
        return y_loc, k_rows.reshape(tok, kv_heads, hd), v_rows.reshape(tok, kv_heads, hd)

    return jax.shard_map(local_fn, mesh=mesh, in_specs=(row_spec, row_spec, row_spec, P(), P(), P(), P()), out_specs=(row_spec, row_spec, row_spec), check_vma=False)
```

```python
import functools

import jax
import jax.numpy as jnp
import numpy as np
from jax import lax
from jax.experimental import pallas as pl
from jax.experimental.pallas import tpu as pltpu
from jax.sharding import PartitionSpec as P

ROPE_BASE = 500000
MESH_ID = pl.DeviceIdType.MESH
NDEV = 8
NEG = -1e30
LOG2E = 1.4426950408889634
KC, VC, QN, KN, VN = range(5)
NBUF = 4


def rope_table(first, count, head_dim):
    f32 = np.float32
    inv_freq = f32(1.0) / (f32(ROPE_BASE) ** (np.arange(0, head_dim, 2, dtype=f32) / f32(head_dim)))
    angles = (first + np.arange(count)).astype(f32)[:, None] * inv_freq[None, :]
    return np.concatenate([np.cos(angles.astype(np.float64)), np.sin(angles.astype(np.float64))], axis=1).astype(f32)


def layer_kernel(group, tok, scale, x_hbm, wq_hbm, wk_hbm, wv_hbm, wo_hbm, table_hbm, kc_hbm, vc_hbm, y_hbm, ko_hbm, vo_hbm,
                 x_s, cos_s, sin_s, wbuf, q_send, k_rows, v_rows, q_s, kc_s, vc_raw, vc_t, kn_s, vn_raw, vn_t, acc, m_s, l_s, s_s, osend, o_s, kc_out, vc_out,
                 in_sem, w_sem, send_sem, recv_sem, osend_sem, orecv_sem):
    y = lax.axis_index('sp')
    xc = lax.axis_index('cp')
    x, c = xc // 2, xc % 2
    me = y * 4 + xc
    c2 = scale * LOG2E
    hd = cos_s.shape[1]
    gw = group * hd
    wide = wbuf.shape[2]

    def peer(k):
        py, px, pc = (y + k // 4) % 2, (x + (k // 2) % 2) % 2, (c + k % 2) % 2
        return py * 4 + px * 2 + pc, (0, py, px * 2 + pc)

    def head_cols(dev):
        return pl.ds(pl.multiple_of(dev * hd, hd), hd)

    def group_cols(dev):
        return pl.ds(pl.multiple_of(dev * gw, gw), gw)

    barrier = pltpu.get_barrier_semaphore()
    for k in range(1, NDEV):
        pl.semaphore_signal(barrier, inc=1, device_id=peer(k)[1], device_id_type=MESH_ID)

    def q_chip(i):
        kc = (i + 1) % 4
        return ((y + kc // 2) % 2) * 2 + (x + kc % 2) % 2

    def w_copy(w_hbm, col, width, t):
        return pltpu.make_async_copy(w_hbm.at[:, pl.ds(pl.multiple_of(col, 256), width)], wbuf.at[t % NBUF, :, pl.ds(0, width)], w_sem.at[t % NBUF])

    def wq_tile(i):
        return w_copy(wq_hbm, q_chip(i) * wide, wide, i)

    def wk_tile(i):
        return w_copy(wk_hbm, i * 512, 512, 4 + i)

    def wv_tile(i):
        return w_copy(wv_hbm, i * 512, 512, 6 + i)

    def wo_tile(n):
        return w_copy(wo_hbm, n * wide, wide, n)

    loads = [pltpu.make_async_copy(x_hbm, x_s, in_sem.at[0]), pltpu.make_async_copy(table_hbm.at[pl.ds(pl.multiple_of(me * tok, tok), tok)], cos_s, in_sem.at[1])]
    raw = [pltpu.make_async_copy(hbm, osend.at[:, :, pl.ds(n * hd, hd)], in_sem.at[2 + n]) for n, hbm in enumerate((kc_hbm, vc_hbm))]
    for cp in raw + loads:
        cp.start()
    wq_tile(0).start()
    wq_tile(1).start()

    def src(kind, dev):
        if kind in (KN, VN):
            return (k_rows if kind == KN else v_rows).at[:, head_cols(dev)]
        return {KC: kc_out, VC: vc_out, QN: q_send}[kind].at[dev]

    dsts = (kc_s, vc_raw, q_s, kn_s, vn_raw)

    def local(kind):
        slot = me if kind in (KN, VN) else 0
        return pltpu.make_async_copy(src(kind, me), dsts[kind].at[slot], recv_sem.at[kind, 0])

    def remote(kind, k):
        p, did = peer(k)
        slot = me if kind in (KN, VN) else k
        return pltpu.make_async_remote_copy(src_ref=src(kind, p), dst_ref=dsts[kind].at[slot], send_sem=send_sem.at[kind, k],
                                            recv_sem=recv_sem.at[kind, k], device_id=did, device_id_type=MESH_ID)

    def arrived(kind, k):
        slot = peer(k)[0] if kind in (KN, VN) else k
        pltpu.make_async_copy(src(kind, 0), dsts[kind].at[slot], recv_sem.at[kind, k]).wait()

    for n, out in enumerate((kc_out, vc_out)):
        raw[n].wait()
        for b in range(NDEV):
            s_s[n, b // 4, b % 4 * tok:(b % 4 + 1) * tok, :] = osend[b, :, n * hd:(n + 1) * hd].astype(jnp.float32)
        for h in range(NDEV):
            for g in range(2):
                out[h, g * tok // 2:(g + 1) * tok // 2, :] = s_s[n, g, pl.ds(h, tok // 2, stride=NDEV), :].astype(jnp.bfloat16)
    pl.semaphore_wait(barrier, NDEV - 1)
    local(KC).start()
    local(VC).start()
    order = (1, 2, 4, 6, 3, 5, 7)
    for k in order:
        for kind in (KC, VC):
            remote(kind, k).start()
    acc[...] = jnp.zeros_like(acc)
    l_s[...] = jnp.zeros_like(l_s)
    m_s[...] = jnp.full(m_s.shape, NEG, jnp.float32)
    for cp in loads:
        cp.wait()
    table = cos_s[...]
    turned = pltpu.roll(table, hd // 2, 1)
    low = lax.broadcasted_iota(jnp.int32, table.shape, 1) < hd // 2
    cos_s[...] = jnp.where(low, table, turned)
    sin_s[...] = jnp.where(low, -turned, table)

    def project(t, n):
        return jnp.dot(x_s[...], wbuf[t % NBUF, :, n * 256:(n + 1) * 256], preferred_element_type=jnp.float32).astype(jnp.bfloat16)

    def rope(rows):
        v = rows.astype(jnp.float32)
        return v * cos_s[...] + pltpu.roll(v, hd // 2, 1) * sin_s[...]

    def q_tile(i, carry):
        @pl.when(jnp.logical_and(i > 0, i < 3))
        def _():
            for core in range(2):
                remote(QN, 2 * i + core).start()

        @pl.when(i < 2)
        def _():
            wq_tile(i + 2).start()

        @pl.when(i >= 2)
        def _():
            wk_tile(i - 2).start()

        wq_tile(i).wait()
        chip = q_chip(i)
        for n in range(wide // 256):
            rows = project(i, n)
            for h in range(2):
                head = 2 * n + h
                r = head % group
                q_send[2 * chip + head // group, r * tok:(r + 1) * tok, :] = (rope(rows[:, h * hd:(h + 1) * hd]) * c2).astype(jnp.bfloat16)
        return carry

    lax.fori_loop(0, 4, q_tile, 0)

    def k_tile(i, carry):
        wv_tile(i).start()
        wk_tile(i).wait()
        for n in range(2):
            rows = project(4 + i, n)
            for h in range(2):
                k_rows[:, head_cols(4 * i + 2 * n + h)] = rope(rows[:, h * hd:(h + 1) * hd]).astype(jnp.bfloat16)

        @pl.when(i == 0)
        def _():
            remote(QN, 1).start()
            local(QN).start()
        return carry

    lax.fori_loop(0, 2, k_tile, 0)

    def v_tile(i, carry):
        wv_tile(i).wait()
        for n in range(2):
            v_rows[:, pl.ds(pl.multiple_of(512 * i + 256 * n, 256), 256)] = project(6 + i, n)

        @pl.when(i == 0)
        def _():
            for k in order:
                remote(KN, k).start()
            local(KN).start()
        return carry

    lax.fori_loop(0, 2, v_tile, 0)
    news = [pltpu.make_async_copy(osend.at[:, :, pl.ds(n * hd, hd)], hbm, in_sem.at[2 + n]) for n, hbm in enumerate((ko_hbm, vo_hbm))]
    for n, rows in enumerate((k_rows, v_rows)):
        for h in range(NDEV):
            for g in range(2):
                s_s[n, g, pl.ds(h, tok // 2, stride=NDEV), :] = rows[g * tok // 2:(g + 1) * tok // 2, h * hd:(h + 1) * hd].astype(jnp.float32)
        for b in range(NDEV):
            osend[b, :, n * hd:(n + 1) * hd] = s_s[n, b // 4, b % 4 * tok:(b % 4 + 1) * tok, :].astype(jnp.bfloat16)

    for n in range(4):
        wo_tile(n).start()
    for k in order:
        remote(VN, k).start()
    for k in (6, 7):
        remote(QN, k).start()
    local(VN).start()
    for cp in news:
        cp.start()
    def qk(keys, k, rows):
        return lax.dot_general(keys, q_s[k, rows, :], (((1,), (1,)), ((), ())), preferred_element_type=jnp.float32)

    def slab(u, j, rows, cols):
        return j % 2, pl.ds((u * (cols // 256) + j // 2) * rows, rows)

    def put(slot, u, val):
        rows, cols = val.shape
        for j in range(cols // 128):
            side, where = slab(u, j, rows, cols)
            s_s[slot, side, where, :] = val[:, j * 128:(j + 1) * 128]

    def get(slot, u, rows, cols):
        parts = []
        for j in range(cols // 128):
            side, where = slab(u, j, rows, cols)
            parts.append(s_s[slot, side, where, :])
        return jnp.concatenate(parts, axis=1)

    def tile_max(old, val):
        top = jnp.max(val, axis=0, keepdims=True)
        return top if old is None else jnp.maximum(old, top)

    def sub_step(slot, k, cols, size, mx, pieces, depth, vt, following):
        m_old = m_s[k, :, cols]
        m_new = jnp.maximum(m_old, mx)
        m_s[k, :, cols] = m_new
        alpha = jnp.exp2(m_old - m_new)
        total, pv, mx_next = None, None, None
        for u in range(pieces):
            s_next = None if following is None else following(u)
            p = jnp.exp2(get(slot, u, depth, size) - m_new)
            if s_next is not None:
                put(1 - slot, u, s_next)
                mx_next = tile_max(mx_next, s_next)
            part = jnp.sum(p, axis=0, keepdims=True)
            prod = jnp.dot(vt(u), p.astype(jnp.bfloat16), preferred_element_type=jnp.float32)
            total = part if total is None else total + part
            pv = prod if pv is None else pv + prod
        l_s[k, :, cols] = l_s[k, :, cols] * alpha + total
        acc[k, :, cols] = acc[k, :, cols] * alpha + pv
        return mx_next

    def first_tile(pieces, scores):
        mx = None
        for u in range(pieces):
            val = scores(u)
            put(0, u, val)
            mx = tile_max(mx, val)
        return mx

    def cache_chunk(j):
        for core in range(2):
            arrived(KC, 2 * j + core)
            arrived(VC, 2 * j + core)
            vc_t[j, :, core * tok:(core + 1) * tok] = vc_raw[2 * j + core].T

    def cache_part(first, count):
        pieces = NDEV // 2
        steps = 2 * count
        mx0 = first_tile(pieces, lambda u: qk(kc_s[u], first, pl.ds(0, 256)))

        def step(t, mx):
            k, half = first + t // 2, t % 2
            tn = jnp.minimum(t + 1, steps - 1)
            k_next, half_next = first + tn // 2, tn % 2
            tiles = group * tok // 256
            for r in range(tiles):
                if r + 1 < tiles:
                    following = lambda u, r=r: qk(kc_s[pieces * half + u], k, pl.ds((r + 1) * 256, 256))
                else:
                    @pl.when(jnp.logical_and(first == 0, t == 0))
                    def _():
                        cache_chunk(2)
                        cache_chunk(3)

                    @pl.when(jnp.logical_and(half == 1, t < steps - 1))
                    def _():
                        arrived(QN, k_next)

                    following = lambda u: qk(kc_s[pieces * half_next + u], k_next, pl.ds(0, 256))
                mx = sub_step(r % 2, k, pl.ds(r * 256, 256), 256, mx, pieces, tok,
                              lambda u: vc_t[2 * half + u // 2, :, (u % 2) * tok:(u % 2 + 1) * tok], following)
            return mx

        lax.fori_loop(0, steps, step, mx0)

    wide_rows = group * tok // 2

    def causal(h, val):
        key = lax.broadcasted_iota(jnp.int32, (tok, wide_rows), 0)
        row = (lax.broadcasted_iota(jnp.int32, (tok, wide_rows), 1) + h * wide_rows) & (tok - 1)
        return jnp.where(key <= row, val, NEG)

    def row_half(h):
        return pl.ds(h * wide_rows, wide_rows)

    def new_block(k, carry):
        arrived(KN, k)
        arrived(VN, k)
        dev = peer(k)[0]
        vn_t[dev] = vn_raw[dev].T
        return carry

    def send_out(k):
        return pltpu.make_async_remote_copy(src_ref=osend.at[k], dst_ref=o_s.at[k // 2, :, group_cols(c)], send_sem=osend_sem.at[k],
                                            recv_sem=orecv_sem.at[k], device_id=peer(k)[1], device_id_type=MESH_ID)

    def out_arrived(k):
        pltpu.make_async_copy(osend.at[k], o_s.at[k // 2, :, group_cols(peer(k)[0] % 2)], orecv_sem.at[k]).wait()

    def item(i):
        return jnp.where(i < 4, 2 + 2 * (i % 2) + i // 2, jnp.where(i < 6, i + 2, NDEV - 1 - i))

    def new_part(i, carry):
        k = item(i)
        p = peer(k)[0]

        @pl.when(jnp.logical_or(i == 0, i // 2 == 2))
        def _():
            @pl.when(i > 0)
            def _():
                arrived(QN, k)

            cache_part((i // 4) * k, jnp.where(i == 0, 6, 1))

        @pl.when(i == 0)
        def _():
            for cp in news:
                cp.wait()
            lax.fori_loop(0, NDEV, new_block, 0)

        mx = first_tile(1, lambda u: causal(0, qk(kn_s[p], k, row_half(0))))
        mx = sub_step(0, k, row_half(0), wide_rows, mx, 1, tok, lambda u: vn_t[p], lambda u: causal(1, qk(kn_s[p], k, row_half(1))))
        mx = sub_step(1, k, row_half(1), wide_rows, mx, 1, tok, lambda u: vn_t[p], lambda u: qk(kn_s[0], k, row_half(0)))

        @pl.when(i > 0)
        def _():
            send_out(item(i - 1)).start()

        def earlier(j, mx):
            jn = jnp.minimum(j + 1, p - 1)
            mx = sub_step(0, k, row_half(0), wide_rows, mx, 1, tok, lambda u: vn_t[j], lambda u: qk(kn_s[j], k, row_half(1)))
            return sub_step(1, k, row_half(1), wide_rows, mx, 1, tok, lambda u: vn_t[j], lambda u: qk(kn_s[jn], k, row_half(0)))

        lax.fori_loop(0, p, earlier, mx)
        for r in range(group):
            cols = slice(r * tok, (r + 1) * tok)
            o_t = acc[k, :, cols] * (1.0 / l_s[k, :, cols])
            osend[k, :, r * hd:(r + 1) * hd] = o_t.T.astype(jnp.bfloat16)
        return carry

    arrived(QN, 0)
    cache_chunk(0)
    cache_chunk(1)
    lax.fori_loop(0, NDEV, new_part, 0)

    own = pltpu.make_async_copy(osend.at[0], o_s.at[0, :, group_cols(c)], orecv_sem.at[0])
    for n in range(4):
        wo_tile(n).wait()
    quarter = tok // 4

    def y_piece(kc, old, last):
        chip = ((y + kc // 2) % 2) * 2 + (x + kc % 2) % 2
        w_rows = pl.ds(pl.multiple_of(chip * wide, wide), wide)

        def tiles(n, carry):
            for sub in range(3):
                val = jnp.dot(o_s[kc], wbuf[n, w_rows, sub * 256:(sub + 1) * 256], preferred_element_type=jnp.float32)
                if old:
                    val = val + jnp.concatenate([acc[2 * n + (4 * sub + u) // 6, :, (4 * sub + u) % 6 * 256:(4 * sub + u) % 6 * 256 + 256] for u in range(4)], axis=0)
                if last:
                    x_s[:, pl.ds(pl.multiple_of(n * wide + sub * 256, 256), 256)] = val.astype(jnp.bfloat16)
                else:
                    for u in range(4):
                        f = 4 * sub + u
                        acc[2 * n + f // 6, :, f % 6 * 256:f % 6 * 256 + 256] = val[u * quarter:(u + 1) * quarter]
            if last:
                @pl.when(n > 0)
                def _():
                    y_copy(n - 1).start()
            return carry

        lax.fori_loop(0, 4, tiles, 0)

    def y_copy(n):
        cols = pl.ds(pl.multiple_of(n * wide, wide), wide)
        return pltpu.make_async_copy(x_s.at[:, cols], y_hbm.at[:, cols], w_sem.at[n])

    out_arrived(2)
    out_arrived(3)
    y_piece(1, False, False)
    own.start()
    out_arrived(4)
    out_arrived(5)
    y_piece(2, True, False)
    out_arrived(1)
    own.wait()
    y_piece(0, True, False)
    out_arrived(6)
    out_arrived(7)
    y_piece(3, True, True)
    for k in range(1, NDEV):
        for kind in range(5):
            remote(kind, k).wait_send()
        send_out(k).wait_send()
    y_copy(3).start()
    for n in range(4):
        y_copy(n).wait()


def layer(x_loc, w_q, w_k, w_v, w_o, table, kc_loc, vc_loc):
    tok, kv_heads, hd = kc_loc.shape
    d_model = x_loc.shape[1]
    group = w_q.shape[1] // (kv_heads * hd)
    rows = group * tok
    bf, f32 = jnp.bfloat16, jnp.float32
    hbm = pl.BlockSpec(memory_space=pl.ANY)
    sds = jax.ShapeDtypeStruct
    dma = pltpu.SemaphoreType.DMA
    return pl.pallas_call(
        functools.partial(layer_kernel, group, tok, hd ** -0.5),
        out_shape=(sds((tok, d_model), bf), sds((kv_heads, tok, hd), bf), sds((kv_heads, tok, hd), bf)),
        in_specs=[hbm] * 8,
        out_specs=(hbm, hbm, hbm),
        scratch_shapes=[
            pltpu.VMEM((tok, d_model), bf),
            pltpu.VMEM((tok, hd), f32),
            pltpu.VMEM((tok, hd), f32),
            pltpu.VMEM((NBUF, d_model, 2 * group * hd), bf),
            pltpu.VMEM((NDEV, rows, hd), bf),
            pltpu.VMEM((tok, kv_heads * hd), bf),
            pltpu.VMEM((tok, kv_heads * hd), bf),
            pltpu.VMEM((NDEV, rows, hd), bf),
            pltpu.VMEM((NDEV, tok, hd), bf),
            pltpu.VMEM((NDEV, tok, hd), bf),
            pltpu.VMEM((NDEV // 2, hd, 2 * tok), bf),
            pltpu.VMEM((NDEV, tok, hd), bf),
            pltpu.VMEM((NDEV, tok, hd), bf),
            pltpu.VMEM((NDEV, hd, tok), bf),
            pltpu.VMEM((NDEV, hd, rows), f32),
            pltpu.VMEM((NDEV, 1, rows), f32),
            pltpu.VMEM((NDEV, 1, rows), f32),
            pltpu.VMEM((2, 2, 4 * tok, 128), f32),
            pltpu.VMEM((NDEV, tok, group * hd), bf),
            pltpu.VMEM((NDEV // 2, tok, 2 * group * hd), bf),
            pltpu.VMEM((NDEV, tok, hd), bf),
            pltpu.VMEM((NDEV, tok, hd), bf),
            dma((4,)),
            dma((NBUF,)),
            dma((5, NDEV)),
            dma((5, NDEV)),
            dma((NDEV,)),
            dma((NDEV,)),
        ],
        compiler_params=pltpu.CompilerParams(collective_id=0, has_side_effects=True, vmem_limit_bytes=63 * 2**20),
        name='head_layer',
    )(x_loc, w_q, w_k, w_v, w_o, table, kc_loc.reshape(kv_heads, tok, hd), vc_loc.reshape(kv_heads, tok, hd))


def solution(mesh):
    seq_size = mesh.shape['sp'] * mesh.shape['cp']
    row_spec = P(('dp', 'sp', 'cp'))

    def local_fn(x_loc, kc_loc, vc_loc, w_q, w_k, w_v, w_o):
        tok, d_model = x_loc.shape
        cache_loc, kv_heads, hd = kc_loc.shape
        table = jnp.asarray(rope_table(cache_loc * seq_size, tok * seq_size, hd))
        y_loc, k_rows, v_rows = layer(x_loc, w_q, w_k, w_v, w_o, table, kc_loc, vc_loc)
        return y_loc, k_rows.reshape(tok, kv_heads, hd), v_rows.reshape(tok, kv_heads, hd)

    return jax.shard_map(local_fn, mesh=mesh, in_specs=(row_spec, row_spec, row_spec, P(), P(), P(), P()), out_specs=(row_spec, row_spec, row_spec), check_vma=False)
```
